32 devices in a mesh: seq: 8 (over z, x), group: 4 (over y, core).
Axes of the slice: x: 2, y: 2, z: 4, core: 2. Of those that a mesh axis runs over, the one named last changes fastest.
Arguments:
- new_queries: bfloat16 [8, 8, 8, 128], P('seq', 'group'), may hold values from -6 to 6
- stored_keys: bfloat16 [8, 8, 4096, 128], P(None, 'group', 'seq'), may hold values from -6 to 6
- stored_values: bfloat16 [8, 8, 4096, 128], P(None, 'group', 'seq'), may hold values from -6 to 6
- used_length: int32 [8], replicated, may hold values from 2048 to 4096
- out_weight: bfloat16 [8, 8, 128, 5120], P('group'), may hold values from -0.0625 to 0.0625
Outputs:
- token_out: bfloat16 [8, 5120], P('seq', 'group')
The draws below stay inside these ranges and needn't reach their ends.
All inputs are finite; a program needn't handle non-finite values.
Results may differ from the reference program's by a relative error of at most 0.0025.
Values may be sent and summed in bfloat16 or wider, within the bound.
A program may use at most 128 MiB of HBM per device.

```python
import jax
import jax.numpy as jnp
from jax import lax

BATCH = 8
LENGTH = 4096
KV_HEADS = 8
GROUP = 8
HEAD_SIZE = 128
D_MODEL = 5120


def plant(drawn, key, smallest, largest):
    place = [jax.random.randint(jax.random.fold_in(key, axis), (), 0, length) for axis, length in enumerate(drawn.shape)]
    longest = drawn.shape.index(max(drawn.shape))
    neighbour = place[:longest] + [(place[longest] + 1) % drawn.shape[longest]] + place[longest + 1:]
    return drawn.at[tuple(place)].set(smallest).at[tuple(neighbour)].set(largest)


def steps_of(rng, extent, shards, smallest, top_value):
    def one(axis_at, shards_of):
        draws = jax.random.uniform(jax.random.fold_in(jax.random.fold_in(rng, 6), axis_at), (shards_of,), jnp.float32, smallest / len(shards), top_value / len(shards))
        return jnp.repeat(jnp.exp(draws), extent[axis_at] // shards_of).reshape((-1,) + (1,) * (len(extent) - axis_at - 1))

    gain = one(*shards[0])
    for cut in shards[1:]:
        gain = gain * one(*cut)
    return gain


def scatter_about(own_key, shape, deviation, reach, split=(), kind=jnp.bfloat16):
    array = jax.random.normal(own_key, shape, jnp.float32) * deviation
    if len(split) > 0:
        array = steps_of(own_key, shape, split, -0.22, 0.18) * array
    return jnp.clip(array, min=-reach, max=reach).astype(kind)


def setup_inputs(seed: int = 0) -> dict:
    arg_keys = jax.random.split(jax.random.key(seed), 6)
    new_queries = scatter_about(arg_keys[0], (BATCH, KV_HEADS, GROUP, HEAD_SIZE), 1.0, 6.0, ((0, 8), (1, 4)))
    stored_keys = scatter_about(arg_keys[1], (BATCH, KV_HEADS, LENGTH, HEAD_SIZE), 1.0, 6.0, ((1, 4), (2, 8)))
    stored_values = scatter_about(arg_keys[2], (BATCH, KV_HEADS, LENGTH, HEAD_SIZE), 1.0, 6.0, ((1, 4), (2, 8)))
    used_length = plant(jax.random.randint(arg_keys[3], (BATCH,), LENGTH // 2, LENGTH + 1), jax.random.fold_in(arg_keys[3], 1), LENGTH // 2, LENGTH).astype(jnp.int32)
    out_weight = scatter_about(arg_keys[4], (KV_HEADS, GROUP, HEAD_SIZE, D_MODEL), (KV_HEADS * GROUP * HEAD_SIZE) ** -0.5, 0.0625, ((0, 4),))
    return {"new_queries": new_queries, "stored_keys": stored_keys, "stored_values": stored_values, "used_length": used_length, "out_weight": out_weight}


def reference(new_queries, stored_keys, stored_values, used_length, out_weight):
    def one_sequence(item):
        query_one, keys_one, values_one, length_one = item
        logit = jnp.einsum("kgd,ktd->kgt", query_one.astype(jnp.float32), keys_one.astype(jnp.float32)) * HEAD_SIZE ** -0.5
        logit = jnp.where(jnp.arange(LENGTH) < length_one, logit, -1e30)
        share = jax.nn.softmax(logit, axis=-1)
        return jnp.einsum("kgt,ktd->kgd", share, values_one.astype(jnp.float32), precision=lax.Precision.HIGHEST)
    read = lax.map(one_sequence, (new_queries, stored_keys, stored_values, used_length)).astype(jnp.bfloat16)
    read = lax.optimization_barrier(read)
    token_out = jnp.einsum("bkgd,kgdm->bm", read.astype(jnp.float32), out_weight.astype(jnp.float32)).astype(jnp.bfloat16)
    return token_out
```

```python
import functools

import jax
import jax.numpy as jnp
from jax import lax
from jax.experimental import pallas as pl
from jax.experimental.pallas import tpu as pltpu
from jax.sharding import PartitionSpec as P

MESH = pl.DeviceIdType.MESH
CLUSTER = 2


def kernel(
    n, ng, cluster, scale,
    q_hbm, k_hbm, v_hbm, used, w_hbm, out_ref,
    q_own, q_all, k_v, v_v, w_v, acc_buf, parts, stat_buf, stats, coef, lhs, term, landed,
    local_sem, k_sem, v_sem, w_sem, q_send, q_recv, s_send, s_recv, a_send, a_recv, t_send, t_recv,
):
    me, mg = lax.axis_index("seq"), lax.axis_index("group")
    batch, heads, stretch, size = k_v.shape
    rows = q_own.shape[0]
    per_head = rows // heads
    rf = rows // cluster
    base, f = (me // cluster) * cluster, lax.rem(me, cluster)
    width = out_ref.shape[1]
    depth = rf * size

    q_load = pltpu.make_async_copy(q_hbm, q_own, local_sem.at[0])
    q_load.start()

    barrier = pltpu.get_barrier_semaphore()
    peers = 0
    for j in range(1, n):
        pl.semaphore_signal(
            barrier, inc=1, device_id={"seq": lax.rem(me + j, n), "group": mg}, device_id_type=MESH
        )
        peers += 1
    for dj in range(cluster):
        for dg in range(1, ng):
            pl.semaphore_signal(
                barrier,
                inc=1,
                device_id={"seq": base + lax.rem(f + dj, cluster), "group": lax.rem(mg + dg, ng)},
                device_id_type=MESH,
            )
            peers += 1

    k_loads = [pltpu.make_async_copy(k_hbm.at[b], k_v.at[b], k_sem.at[b]) for b in range(batch)]
    v_loads = [pltpu.make_async_copy(v_hbm.at[b], v_v.at[b], v_sem.at[b]) for b in range(batch)]
    w_row = pl.multiple_of(f * depth, depth)
    w_loads = [
        pltpu.make_async_copy(
            w_hbm.at[pl.ds(w_row, depth), pl.ds(g * width, width)], w_v.at[g], w_sem.at[g]
        )
        for g in range(ng)
    ]
    for load in k_loads + v_loads + w_loads:
        load.start()

    q_load.wait()
    q_keep = pltpu.make_async_copy(q_own, q_all.at[me], local_sem.at[1])
    q_keep.start()
    pl.semaphore_wait(barrier, peers)

    def to_seq(src, dst, send, recv, j):
        return pltpu.make_async_remote_copy(
            src_ref=src, dst_ref=dst, send_sem=send.at[j], recv_sem=recv.at[j],
            device_id={"seq": lax.rem(me + j, n), "group": mg}, device_id_type=MESH,
        )

    q_out = [to_seq(q_own, q_all.at[me], q_send, q_recv, j) for j in range(1, n)]
    for copy in q_out:
        copy.start()
    lhs[...] = jnp.zeros_like(lhs)
    for load in k_loads:
        load.wait()
    q_keep.wait()
    for copy in q_out:
        copy.wait_recv()

    place = me * stretch + lax.broadcasted_iota(jnp.int32, (rows, stretch), 1)
    shares, tops, sums = [], [], []
    for b in range(batch):
        q = q_all[b]
        split_q = jnp.concatenate(
            [
                jnp.where(lax.broadcasted_iota(jnp.int32, (rows, size), 0) // per_head == h, q, jnp.zeros_like(q))
                for h in range(heads)
            ],
            axis=1,
        )
        keys = jnp.concatenate([k_v[b, h] for h in range(heads)], axis=1)
        logit = lax.dot_general(
            split_q, keys, (((1,), (1,)), ((), ())), preferred_element_type=jnp.float32
        ) * scale
        filled = place < used[b]
        logit = jnp.where(filled, logit, -1e30)
        top = jnp.max(logit, axis=1, keepdims=True)
        part = jnp.where(filled, jnp.exp(logit - top), 0.0)
        tops.append(top)
        sums.append(jnp.sum(part, axis=1, keepdims=True))
        shares.append(part)

    all_tops = jnp.concatenate(tops, axis=0)
    all_sums = jnp.concatenate(sums, axis=0)
    lane = lax.broadcasted_iota(jnp.int32, (batch * rows, 128), 1)
    stat_buf[...] = jnp.where(lane == 0, all_tops, all_sums).T[:2]
    s_out = [to_seq(stat_buf, stats.at[me], s_send, s_recv, j) for j in range(1, n)]
    for copy in s_out:
        copy.start()
    s_keep = pltpu.make_async_copy(stat_buf, stats.at[me], local_sem.at[2])
    s_keep.start()

    for load in v_loads:
        load.wait()
    for b in range(batch):
        part = shares[b]
        high = part.astype(jnp.bfloat16)
        low = (part - high.astype(jnp.float32)).astype(jnp.bfloat16)
        values = jnp.concatenate([v_v[b, h] for h in range(heads)], axis=1)
        both = jnp.dot(
            jnp.concatenate([high, low], axis=0), values, preferred_element_type=jnp.float32
        )
        both = both[:rows] + both[rows:]
        read = jnp.concatenate(
            [
                both[h * per_head : (h + 1) * per_head, h * size : (h + 1) * size]
                for h in range(heads)
            ],
            axis=0,
        )
        c, at = b // cluster, b % cluster
        for piece in range(cluster):
            acc_buf[c * cluster + piece, at * rf : (at + 1) * rf] = read[piece * rf : (piece + 1) * rf]

    a_out = [
        to_seq(acc_buf.at[lax.rem(me + j, n)], parts.at[me], a_send, a_recv, j) for j in range(1, n)
    ]
    for copy in a_out:
        copy.start()
    a_keep = pltpu.make_async_copy(acc_buf.at[me], parts.at[me], local_sem.at[3])
    a_keep.start()

    s_keep.wait()
    for copy in s_out:
        copy.wait_recv()
    m_all, s_all = stats[:, 0, :], stats[:, 1, :]
    weight = jnp.exp(m_all - jnp.max(m_all, axis=0, keepdims=True))
    weight = weight / jnp.sum(weight * s_all, axis=0, keepdims=True)
    weight = jnp.concatenate([weight, jnp.zeros((128 - n, batch * rows), jnp.float32)], axis=0)
    coef[...] = weight.T
    own = jnp.concatenate(
        [coef[pl.ds(pl.multiple_of((base + at) * rows + f * rf, rf), rf)] for at in range(cluster)],
        axis=0,
    )
    a_keep.wait()
    for copy in a_out:
        copy.wait_recv()
    read = own[:, 0:1] * parts[0]
    for src in range(1, n):
        read += own[:, src : src + 1] * parts[src]
    for at in range(cluster):
        for r in range(rf):
            lhs[at : at + 1, r * size : (r + 1) * size] = read[at * rf + r : at * rf + r + 1]
    token = lhs[...].astype(jnp.bfloat16)

    for load in w_loads:
        load.wait()
    t_out = []
    for dg in [*range(1, ng), 0]:
        g = lax.rem(mg + dg, ng)
        out = jnp.dot(token, w_v[g], preferred_element_type=jnp.float32)
        for at in range(cluster):
            term[g, at] = out[at : at + 1]
        for dj in range(cluster):
            at = lax.rem(f + dj, cluster)
            slot = f * ng + mg
            if dg == 0 and dj == 0:
                t_keep = pltpu.make_async_copy(term.at[g, at], landed.at[slot], local_sem.at[4])
                t_keep.start()
                continue
            copy = pltpu.make_async_remote_copy(
                src_ref=term.at[g, at], dst_ref=landed.at[slot],
                send_sem=t_send.at[dj * ng + dg], recv_sem=t_recv.at[dj * ng + dg],
                device_id={"seq": base + at, "group": g}, device_id_type=MESH,
            )
            copy.start()
            t_out.append(copy)
    t_keep.wait()
    for copy in t_out:
        copy.wait_recv()
    total = landed[0]
    for slot in range(1, cluster * ng):
        total += landed[slot]
    out_ref[...] = total.astype(out_ref.dtype)
    for copy in q_out + s_out + a_out + t_out:
        copy.wait_send()


def solution(mesh):
    n, ng = mesh.shape["seq"], mesh.shape["group"]

    def per_device(new_queries, stored_keys, stored_values, used_length, out_weight):
        batch, heads, stretch, size = stored_keys.shape
        group = new_queries.shape[2]
        rows = heads * group
        model = out_weight.shape[-1]
        cluster, width = CLUSTER, model // ng
        rf = rows // cluster
        dma = pltpu.SemaphoreType.DMA
        anywhere = pl.BlockSpec(memory_space=pl.ANY)
        f32, bf16 = jnp.float32, jnp.bfloat16
        return pl.pallas_call(
            functools.partial(kernel, n, ng, cluster, size ** (-0.5)),
            out_shape=jax.ShapeDtypeStruct((1, width), bf16),
            in_specs=[anywhere, anywhere, anywhere, pl.BlockSpec(memory_space=pltpu.SMEM), anywhere],
            out_specs=pl.BlockSpec(memory_space=pltpu.VMEM),
            scratch_shapes=[
                pltpu.VMEM((rows, size), bf16),
                pltpu.VMEM((n, rows, size), bf16),
                pltpu.VMEM(stored_keys.shape, bf16),
                pltpu.VMEM(stored_values.shape, bf16),
                pltpu.VMEM((ng, rf * size, width), bf16),
                pltpu.VMEM((n, rows, size), f32),
                pltpu.VMEM((n, rows, size), f32),
                pltpu.VMEM((2, batch * rows), f32),
                pltpu.VMEM((n, 2, batch * rows), f32),
                pltpu.VMEM((batch * rows, 128), f32),
                pltpu.VMEM((8, rf * size), f32),
                pltpu.VMEM((ng, cluster, 1, width), f32),
                pltpu.VMEM((cluster * ng, 1, width), f32),
                dma((5,)), dma((batch,)), dma((batch,)), dma((ng,)),
                dma((n,)), dma((n,)), dma((n,)), dma((n,)), dma((n,)), dma((n,)),
                dma((cluster * ng,)), dma((cluster * ng,)),
            ],
            compiler_params=pltpu.CompilerParams(collective_id=0, has_side_effects=True),
        )(
            new_queries.reshape(rows, size),
            stored_keys,
            stored_values,
            used_length,
            out_weight.reshape(rows * size, model),
        )

    return jax.shard_map(
        per_device,
        mesh=mesh,
        in_specs=(
            P("seq", "group", None, None),
            P(None, "group", "seq", None),
            P(None, "group", "seq", None),
            P(),
            P("group", None, None, None),
        ),
        out_specs=P("seq", "group"),
        check_vma=False,
    )
```

```python
import functools

import jax
import jax.numpy as jnp
from jax import lax
from jax.experimental import pallas as pl
from jax.experimental.pallas import tpu as pltpu
from jax.sharding import PartitionSpec as P

MESH = pl.DeviceIdType.MESH
CLUSTER = 2


def kernel(
    n, ng, cluster, scale,
    q_hbm, k_hbm, v_hbm, used, w_hbm, out_ref,
    q_own, q_all, k_v, v_v, w_v, acc_buf, parts, stat_buf, stats, coef, lhs, term, landed,
    local_sem, k_sem, v_sem, w_sem, q_send, q_recv, s_send, s_recv, a_send, a_recv, t_send, t_recv,
):
    me, mg = lax.axis_index("seq"), lax.axis_index("group")
    batch, heads, stretch, size = k_v.shape
    rows = q_own.shape[0]
    per_head = rows // heads
    rf = rows // cluster
    base, f = (me // cluster) * cluster, lax.rem(me, cluster)
    width = out_ref.shape[1]
    depth = rf * size

    q_load = pltpu.make_async_copy(q_hbm, q_own, local_sem.at[0])
    q_load.start()

    barrier = pltpu.get_barrier_semaphore()
    peers = 0
    for j in range(1, n):
        pl.semaphore_signal(
            barrier, inc=1, device_id={"seq": lax.rem(me + j, n), "group": mg}, device_id_type=MESH
        )
        peers += 1
    for dj in range(cluster):
        for dg in range(1, ng):
            pl.semaphore_signal(
                barrier,
                inc=1,
                device_id={"seq": base + lax.rem(f + dj, cluster), "group": lax.rem(mg + dg, ng)},
                device_id_type=MESH,
            )
            peers += 1

    k_loads = [pltpu.make_async_copy(k_hbm.at[b], k_v.at[b], k_sem.at[b]) for b in range(batch)]
    v_loads = [pltpu.make_async_copy(v_hbm.at[b], v_v.at[b], v_sem.at[b]) for b in range(batch)]
    w_row = pl.multiple_of(f * depth, depth)
    w_loads = [
        pltpu.make_async_copy(
            w_hbm.at[pl.ds(w_row, depth), pl.ds(g * width, width)], w_v.at[g], w_sem.at[g]
        )
        for g in range(ng)
    ]
    for load in k_loads + v_loads + w_loads:
        load.start()

    q_load.wait()
    q_keep = pltpu.make_async_copy(q_own, q_all.at[me], local_sem.at[1])
    q_keep.start()
    pl.semaphore_wait(barrier, peers)

    def to_seq(src, dst, send, recv, j):
        return pltpu.make_async_remote_copy(
            src_ref=src, dst_ref=dst, send_sem=send.at[j], recv_sem=recv.at[j],
            device_id={"seq": lax.rem(me + j, n), "group": mg}, device_id_type=MESH,
        )

    q_out = [to_seq(q_own, q_all.at[me], q_send, q_recv, j) for j in range(1, n)]
    for copy in q_out:
        copy.start()
    lhs[...] = jnp.zeros_like(lhs)
    for load in k_loads:
        load.wait()
    q_keep.wait()
    for copy in q_out:
        copy.wait_recv()

    place = me * stretch + lax.broadcasted_iota(jnp.int32, (rows, stretch), 1)
    shares, tops, sums = [], [], []
    for b in range(batch):
        q = q_all[b]
        split_q = jnp.concatenate(
            [
                jnp.where(lax.broadcasted_iota(jnp.int32, (rows, size), 0) // per_head == h, q, jnp.zeros_like(q))
                for h in range(heads)
            ],
            axis=1,
        )
        keys = jnp.concatenate([k_v[b, h] for h in range(heads)], axis=1)
        logit = lax.dot_general(
            split_q, keys, (((1,), (1,)), ((), ())), preferred_element_type=jnp.float32
        ) * scale
        filled = place < used[b]
        logit = jnp.where(filled, logit, -1e30)
        top = jnp.max(logit, axis=1, keepdims=True)
        part = jnp.where(filled, jnp.exp(logit - top), 0.0)
        tops.append(top)
        sums.append(jnp.sum(part, axis=1, keepdims=True))
        shares.append(part)

    all_tops = jnp.concatenate(tops, axis=0)
    all_sums = jnp.concatenate(sums, axis=0)
    lane = lax.broadcasted_iota(jnp.int32, (batch * rows, 128), 1)
    stat_buf[...] = jnp.where(lane == 0, all_tops, all_sums).T[:2]
    s_out = [to_seq(stat_buf, stats.at[me], s_send, s_recv, j) for j in range(1, n)]
    for copy in s_out:
        copy.start()
    s_keep = pltpu.make_async_copy(stat_buf, stats.at[me], local_sem.at[2])
    s_keep.start()

    for load in v_loads:
        load.wait()
    for b in range(batch):
        part = shares[b]
        high = part.astype(jnp.bfloat16)
        low = (part - high.astype(jnp.float32)).astype(jnp.bfloat16)
        values = jnp.concatenate([v_v[b, h] for h in range(heads)], axis=1)
        both = jnp.dot(
            jnp.concatenate([high, low], axis=0), values, preferred_element_type=jnp.float32
        )
        both = both[:rows] + both[rows:]
        read = jnp.concatenate(
            [
                both[h * per_head : (h + 1) * per_head, h * size : (h + 1) * size]
                for h in range(heads)
            ],
            axis=0,
        )
        c, at = b // cluster, b % cluster
        for piece in range(cluster):
            acc_buf[c * cluster + piece, at * rf : (at + 1) * rf] = read[piece * rf : (piece + 1) * rf]

    a_out = [
        to_seq(acc_buf.at[lax.rem(me + j, n)], parts.at[me], a_send, a_recv, j) for j in range(1, n)
    ]
    for copy in a_out:
        copy.start()
    a_keep = pltpu.make_async_copy(acc_buf.at[me], parts.at[me], local_sem.at[3])
    a_keep.start()

    s_keep.wait()
    for copy in s_out:
        copy.wait_recv()
    m_all, s_all = stats[:, 0, :], stats[:, 1, :]
    weight = jnp.exp(m_all - jnp.max(m_all, axis=0, keepdims=True))
    weight = weight / jnp.sum(weight * s_all, axis=0, keepdims=True)
    weight = jnp.concatenate([weight, jnp.zeros((128 - n, batch * rows), jnp.float32)], axis=0)
    coef[...] = weight.T
    own = jnp.concatenate(
        [coef[pl.ds(pl.multiple_of((base + at) * rows + f * rf, rf), rf)] for at in range(cluster)],
        axis=0,
    )
    a_keep.wait()
    for copy in a_out:
        copy.wait_recv()
    read = own[:, 0:1] * parts[0]
    for src in range(1, n):
        read += own[:, src : src + 1] * parts[src]
    for at in range(cluster):
        for r in range(rf):
            lhs[at : at + 1, r * size : (r + 1) * size] = read[at * rf + r : at * rf + r + 1]
    token = lhs[...].astype(jnp.bfloat16)

    for load in w_loads:
        load.wait()
    t_out = []
    for dg in [*range(1, ng), 0]:
        g = lax.rem(mg + dg, ng)
        out = jnp.dot(token, w_v[g], preferred_element_type=jnp.float32)
        for at in range(cluster):
            term[g, at] = out[at : at + 1]
        for dj in range(cluster):
            at = lax.rem(f + dj, cluster)
            slot = f * ng + mg
            if dg == 0 and dj == 0:
                t_keep = pltpu.make_async_copy(term.at[g, at], landed.at[slot], local_sem.at[4])
                t_keep.start()
                continue
            copy = pltpu.make_async_remote_copy(
                src_ref=term.at[g, at], dst_ref=landed.at[slot],
                send_sem=t_send.at[dj * ng + dg], recv_sem=t_recv.at[dj * ng + dg],
                device_id={"seq": base + at, "group": g}, device_id_type=MESH,
            )
            copy.start()
            t_out.append(copy)
    t_keep.wait()
    for copy in t_out:
        copy.wait_recv()
    total = landed[0]
    for slot in range(1, cluster * ng):
        total += landed[slot]
    out_ref[...] = total.astype(out_ref.dtype)
    for copy in q_out + s_out + a_out + t_out:
        copy.wait_send()


def solution(mesh):
    n, ng = mesh.shape["seq"], mesh.shape["group"]

    def per_device(new_queries, stored_keys, stored_values, used_length, out_weight):
        batch, heads, stretch, size = stored_keys.shape
        group = new_queries.shape[2]
        rows = heads * group
        model = out_weight.shape[-1]
        cluster, width = CLUSTER, model // ng
        rf = rows // cluster
        dma = pltpu.SemaphoreType.DMA
        anywhere = pl.BlockSpec(memory_space=pl.ANY)
        f32, bf16 = jnp.float32, jnp.bfloat16
        return pl.pallas_call(
            functools.partial(kernel, n, ng, cluster, size ** (-0.5)),
            out_shape=pltpu.VMEM((1, width), bf16),
            in_specs=[anywhere, anywhere, anywhere, pl.BlockSpec(memory_space=pltpu.SMEM), anywhere],
            out_specs=pl.BlockSpec(memory_space=pltpu.VMEM),
            scratch_shapes=[
                pltpu.VMEM((rows, size), bf16),
                pltpu.VMEM((n, rows, size), bf16),
                pltpu.VMEM(stored_keys.shape, bf16),
                pltpu.VMEM(stored_values.shape, bf16),
                pltpu.VMEM((ng, rf * size, width), bf16),
                pltpu.VMEM((n, rows, size), f32),
                pltpu.VMEM((n, rows, size), f32),
                pltpu.VMEM((2, batch * rows), f32),
                pltpu.VMEM((n, 2, batch * rows), f32),
                pltpu.VMEM((batch * rows, 128), f32),
                pltpu.VMEM((8, rf * size), f32),
                pltpu.VMEM((ng, cluster, 1, width), f32),
                pltpu.VMEM((cluster * ng, 1, width), f32),
                dma((5,)), dma((batch,)), dma((batch,)), dma((ng,)),
                dma((n,)), dma((n,)), dma((n,)), dma((n,)), dma((n,)), dma((n,)),
                dma((cluster * ng,)), dma((cluster * ng,)),
            ],
            compiler_params=pltpu.CompilerParams(collective_id=0, has_side_effects=True),
        )(
            new_queries.reshape(rows, size),
            stored_keys,
            stored_values,
            used_length,
            out_weight.reshape(rows * size, model),
        )

    return jax.shard_map(
        per_device,
        mesh=mesh,
        in_specs=(
            P("seq", "group", None, None),
            P(None, "group", "seq", None),
            P(None, "group", "seq", None),
            P(),
            P("group", None, None, None),
        ),
        out_specs=P("seq", "group"),
        check_vma=False,
    )
```

```python
import functools

import jax
import jax.numpy as jnp
from jax import lax
from jax.experimental import pallas as pl
from jax.experimental.pallas import tpu as pltpu
from jax.sharding import PartitionSpec as P

MESH = pl.DeviceIdType.MESH
CLUSTER = 2


def flip(index, bits):
    out, bit = index, 1
    while bit <= bits:
        if bits & bit:
            out = out + bit - 2 * bit * lax.rem(index // bit, 2)
        bit *= 2
    return out


def kernel(
    n, ng, cluster, scale,
    q_hbm, k_hbm, v_hbm, used, w_hbm, out_ref,
    q_all, k_v, v_v, w_v, made, parts, lhs, term, landed,
    q_sem, k_sem, v_sem, w_sem, q_send, q_recv, a_send, a_recv, t_send, t_recv,
):
    me, mg = lax.axis_index("seq"), lax.axis_index("group")
    batch, heads, stretch, size = k_v.shape
    rows = q_all.shape[1]
    per_head = rows // heads
    rf = rows // cluster
    f = lax.rem(me, cluster)
    width = out_ref.shape[1]
    depth = rf * size

    q_load = pltpu.make_async_copy(q_hbm, q_all.at[0], q_sem)
    q_load.start()
    barrier = pltpu.get_barrier_semaphore()
    partners = [(j, 0) for j in range(1, n)]
    partners += [(t, dg) for t in range(cluster) for dg in range(1, ng)]
    for j, dg in partners:
        pl.semaphore_signal(
            barrier, inc=1, device_id={"seq": flip(me, j), "group": flip(mg, dg)}, device_id_type=MESH
        )

    k_load = pltpu.make_async_copy(k_hbm, k_v, k_sem)
    v_load = pltpu.make_async_copy(v_hbm, v_v, v_sem)
    w_row = pl.multiple_of(f * depth, depth)
    w_loads = [
        pltpu.make_async_copy(
            w_hbm.at[pl.ds(w_row, depth), pl.ds(pl.multiple_of(flip(mg, dg) * width, width), width)],
            w_v.at[dg],
            w_sem.at[dg],
        )
        for dg in range(ng)
    ]
    for load in [k_load, v_load] + w_loads:
        load.start()
    lhs[...] = jnp.zeros_like(lhs)
    place = me * stretch + lax.broadcasted_iota(jnp.int32, (rows, stretch), 1)
    head_of = lax.broadcasted_iota(jnp.int32, (rows, size), 0) // per_head
    lane = lax.broadcasted_iota(jnp.int32, (rows, size), 1)

    def to_seq(src, dst, send, recv, j):
        return pltpu.make_async_remote_copy(
            src_ref=src, dst_ref=dst, send_sem=send.at[j], recv_sem=recv.at[j],
            device_id={"seq": flip(me, j), "group": mg}, device_id_type=MESH,
        )

    q_load.wait()
    pl.semaphore_wait(barrier, len(partners))
    q_out = [to_seq(q_all.at[0], q_all.at[j], q_send, q_recv, j) for j in range(1, n)]
    for copy in q_out[::-1]:
        copy.start()
    k_load.wait()
    v_load.wait()

    a_out = []
    for c in range(n // cluster):
        for i in range(cluster):
            j = c * cluster + i
            if j:
                q_out[j - 1].wait_recv()
        for i in range(cluster):
            j = c * cluster + i
            b = flip(me, j)
            q = q_all[j]
            split_q = jnp.concatenate(
                [jnp.where(head_of == h, q, jnp.zeros_like(q)) for h in range(heads)], axis=1
            )
            keys = jnp.concatenate([k_v[b, h] for h in range(heads)], axis=1)
            logit = lax.dot_general(
                split_q, keys, (((1,), (1,)), ((), ())), preferred_element_type=jnp.float32
            ) * scale
            filled = place < used[b]
            logit = jnp.where(filled, logit, -1e30)
            top = jnp.max(logit, axis=1, keepdims=True).astype(jnp.bfloat16).astype(jnp.float32)
            part = jnp.where(filled, jnp.exp(logit - top), 0.0)
            weight_sum = jnp.sum(part, axis=1, keepdims=True)
            high = part.astype(jnp.bfloat16)
            low = (part - high.astype(jnp.float32)).astype(jnp.bfloat16)
            values = jnp.concatenate([v_v[b, h] for h in range(heads)], axis=1)
            both = jnp.dot(
                jnp.concatenate([high, low], axis=0), values, preferred_element_type=jnp.float32
            )
            both = both[:rows] + both[rows:]
            read = jnp.concatenate(
                [
                    both[h * per_head : (h + 1) * per_head, h * size : (h + 1) * size]
                    for h in range(heads)
                ],
                axis=0,
            )
            read_high = read.astype(jnp.bfloat16).astype(jnp.float32)
            sum_high = weight_sum.astype(jnp.bfloat16).astype(jnp.float32)
            stat = jnp.where(lane == 0, top, jnp.where(lane == 1, sum_high, weight_sum - sum_high))
            for kind, tile in enumerate((read_high, read - read_high, stat)):
                for piece in range(cluster):
                    made[c, piece, kind, i * rf : (i + 1) * rf] = tile[
                        piece * rf : (piece + 1) * rf
                    ].astype(jnp.bfloat16)
        for i in range(cluster):
            j = c * cluster + i
            if j:
                copy = to_seq(made.at[c, flip(f, i)], parts.at[j], a_send, a_recv, j)
                copy.start()
                a_out.append(copy)

    def arranged(tile, p):
        tile = tile.astype(jnp.float32)
        return jnp.concatenate(
            [tile[(t ^ p) * rf : ((t ^ p) + 1) * rf] for t in range(cluster)], axis=0
        )

    got = [[arranged(made[0, f, kind], 0) for kind in range(3)]]
    for j in range(1, n):
        a_out[j - 1].wait_recv()
    for j in range(1, n):
        got.append([arranged(parts[j, kind], j % cluster) for kind in range(3)])
    best = functools.reduce(jnp.maximum, [stat[:, 0:1] for _, _, stat in got])
    weights = [jnp.exp(stat[:, 0:1] - best) for _, _, stat in got]
    total_weight = sum(w * (stat[:, 1:2] + stat[:, 2:3]) for w, (_, _, stat) in zip(weights, got))
    read = sum(w * (high + low) for w, (high, low, _) in zip(weights, got)) / total_weight
    for t in range(cluster):
        for r in range(rf):
            lhs[t : t + 1, r * size : (r + 1) * size] = read[t * rf + r : t * rf + r + 1]
    token = lhs[...].astype(jnp.bfloat16)

    for load in w_loads:
        load.wait()
    t_out = []
    for dg in reversed(range(ng)):
        out = jnp.dot(token, w_v[dg], preferred_element_type=jnp.float32)
        for t in range(cluster):
            if t == 0 and dg == 0:
                own = out[:1]
                continue
            slot = t * ng + dg
            term[slot] = out[t : t + 1]
            copy = pltpu.make_async_remote_copy(
                src_ref=term.at[slot], dst_ref=landed.at[slot],
                send_sem=t_send.at[slot], recv_sem=t_recv.at[slot],
                device_id={"seq": flip(me, t), "group": flip(mg, dg)}, device_id_type=MESH,
            )
            copy.start()
            t_out.append(copy)
    for copy in t_out:
        copy.wait_recv()
    for slot in range(1, cluster * ng):
        own += landed[slot]
    out_ref[...] = own.astype(out_ref.dtype)
    for copy in q_out + a_out + t_out:
        copy.wait_send()


def solution(mesh):
    n, ng = mesh.shape["seq"], mesh.shape["group"]

    def per_device(new_queries, stored_keys, stored_values, used_length, out_weight):
        batch, heads, stretch, size = stored_keys.shape
        group = new_queries.shape[2]
        rows = heads * group
        model = out_weight.shape[-1]
        cluster, width = CLUSTER, model // ng
        rf = rows // cluster
        dma = pltpu.SemaphoreType.DMA
        anywhere = pl.BlockSpec(memory_space=pl.ANY)
        f32, bf16 = jnp.float32, jnp.bfloat16
        return pl.pallas_call(
            functools.partial(kernel, n, ng, cluster, size ** (-0.5)),
            out_shape=pltpu.VMEM((1, width), bf16),
            in_specs=[anywhere, anywhere, anywhere, pl.BlockSpec(memory_space=pltpu.SMEM), anywhere],
            out_specs=pl.BlockSpec(memory_space=pltpu.VMEM),
            scratch_shapes=[
                pltpu.VMEM((n, rows, size), bf16),
                pltpu.VMEM(stored_keys.shape, bf16),
                pltpu.VMEM(stored_values.shape, bf16),
                pltpu.VMEM((ng, rf * size, width), bf16),
                pltpu.VMEM((n // cluster, cluster, 3, cluster * rf, size), bf16),
                pltpu.VMEM((n, 3, cluster * rf, size), bf16),
                pltpu.VMEM((8, rf * size), f32),
                pltpu.VMEM((cluster * ng, 1, width), f32),
                pltpu.VMEM((cluster * ng, 1, width), f32),
                dma, dma, dma, dma((ng,)),
                dma((n,)), dma((n,)), dma((n,)), dma((n,)),
                dma((cluster * ng,)), dma((cluster * ng,)),
            ],
            compiler_params=pltpu.CompilerParams(collective_id=0, has_side_effects=True),
        )(
            new_queries.reshape(rows, size),
            stored_keys,
            stored_values,
            used_length,
            out_weight.reshape(rows * size, model),
        )

    return jax.shard_map(
        per_device,
        mesh=mesh,
        in_specs=(
            P("seq", "group", None, None),
            P(None, "group", "seq", None),
            P(None, "group", "seq", None),
            P(),
            P("group", None, None, None),
        ),
        out_specs=P("seq", "group"),
        check_vma=False,
    )
```

```python
import functools

import jax
import jax.numpy as jnp
from jax import lax
from jax.experimental import pallas as pl
from jax.experimental.pallas import tpu as pltpu
from jax.sharding import PartitionSpec as P

MESH = pl.DeviceIdType.MESH
CLUSTER = 2
CHUNK = 1


def flip(index, bits):
    out, bit = index, 1
    while bit <= bits:
        if bits & bit:
            out = out + bit - 2 * bit * lax.rem(index // bit, 2)
        bit *= 2
    return out


def kernel(
    n, ng, cluster, scale,
    q_hbm, k_hbm, v_hbm, used, w_hbm, out_ref,
    q_all, k_v, v_v, w_v, made, parts, stat_made, stats, lhs, term, landed,
    q_sem, k_sem, v_sem, w_sem, q_send, q_recv, s_send, s_recv, a_send, a_recv, t_send, t_recv,
):
    me, mg = lax.axis_index("seq"), lax.axis_index("group")
    batch, heads, stretch, size = k_v.shape
    rows = q_all.shape[1]
    per_head = rows // heads
    rf = rows // cluster
    f = lax.rem(me, cluster)
    width = out_ref.shape[1]
    depth = rf * size

    q_load = pltpu.make_async_copy(q_hbm, q_all.at[0], q_sem)
    q_load.start()
    barrier = pltpu.get_barrier_semaphore()
    partners = [(j, 0) for j in range(1, n)]
    partners += [(t, dg) for t in range(cluster) for dg in range(1, ng)]
    for j, dg in reversed(partners):
        pl.semaphore_signal(
            barrier, inc=1, device_id={"seq": flip(me, j), "group": flip(mg, dg)}, device_id_type=MESH
        )

    k_load = pltpu.make_async_copy(k_hbm, k_v, k_sem)
    v_load = pltpu.make_async_copy(v_hbm, v_v, v_sem)
    w_row = pl.multiple_of(f * depth, depth)
    w_loads = [
        pltpu.make_async_copy(
            w_hbm.at[pl.ds(w_row, depth), pl.ds(pl.multiple_of(flip(mg, dg) * width, width), width)],
            w_v.at[dg],
            w_sem.at[dg],
        )
        for dg in range(ng)
    ]
    for load in [k_load, v_load] + w_loads:
        load.start()
    lhs[...] = jnp.zeros_like(lhs)
    place = me * stretch + lax.broadcasted_iota(jnp.int32, (rows, stretch), 1)
    head_of = lax.broadcasted_iota(jnp.int32, (rows, size), 0) // per_head
    lane = lax.broadcasted_iota(jnp.int32, (rows, size), 1)
    line, half = lax.broadcasted_iota(jnp.int32, (rows, size), 0), size // 2

    def to_seq(src, dst, send, recv, j):
        return pltpu.make_async_remote_copy(
            src_ref=src, dst_ref=dst, send_sem=send.at[j], recv_sem=recv.at[j],
            device_id={"seq": flip(me, j), "group": mg}, device_id_type=MESH,
        )

    q_load.wait()
    pl.semaphore_wait(barrier, len(partners))
    q_out = [to_seq(q_all.at[0], q_all.at[j], q_send, q_recv, j) for j in range(1, n)]
    for copy in q_out[::-1]:
        copy.start()
    k_load.wait()
    v_load.wait()

    a_out, s_out = [], []
    clusters = n // cluster
    for start in range(0, clusters, CHUNK):
        chunk = range(start, min(start + CHUNK, clusters))
        members = [c * cluster + i for c in chunk for i in range(cluster)]
        for j in members:
            if j:
                q_out[j - 1].wait_recv()
        logits, parts_of, tops, sums, reads = {}, {}, {}, {}, {}
        for j in members:
            b = flip(me, j)
            q = q_all[j]
            split_q = jnp.concatenate(
                [jnp.where(head_of == h, q, jnp.zeros_like(q)) for h in range(heads)], axis=1
            )
            keys = jnp.concatenate([k_v[b, h] for h in range(heads)], axis=1)
            logit = lax.dot_general(
                split_q, keys, (((1,), (1,)), ((), ())), preferred_element_type=jnp.float32
            ) * scale
            logits[j] = jnp.where(place < used[b], logit, -1e30)
        for j in members:
            tops[j] = jnp.max(logits[j], axis=1, keepdims=True)
        for j in members:
            filled = place < used[flip(me, j)]
            part = jnp.where(filled, jnp.exp(logits[j] - tops[j]), 0.0)
            high = part.astype(jnp.bfloat16)
            low = (part - high.astype(jnp.float32)).astype(jnp.bfloat16)
            parts_of[j] = jnp.concatenate([high, low], axis=0)
            sums[j] = jnp.sum(part, axis=1, keepdims=True)
        for j in members:
            b = flip(me, j)
            values = jnp.concatenate([v_v[b, h] for h in range(heads)], axis=1)
            both = jnp.dot(parts_of[j], values, preferred_element_type=jnp.float32)
            both = both[:rows] + both[rows:]
            reads[j] = jnp.concatenate(
                [
                    both[h * per_head : (h + 1) * per_head, h * size : (h + 1) * size]
                    for h in range(heads)
                ],
                axis=0,
            )
        for c in reversed(chunk):
            for piece in range(cluster):
                cut = slice(piece * rf, (piece + 1) * rf)
                pick = [c * cluster + i for i in range(cluster)]
                top = jnp.concatenate([tops[j][cut] for j in pick], axis=0)
                weight_sum = jnp.concatenate([sums[j][cut] for j in pick], axis=0)
                spread = jnp.where(lane == line, top, jnp.where(lane == line + half, weight_sum, 0.0))
                stat_made[c, piece] = jnp.sum(spread, axis=0, keepdims=True)
            for i in reversed(range(cluster)):
                j = c * cluster + i
                if j:
                    s_out.append(to_seq(stat_made.at[c, flip(f, i)], stats.at[j], s_send, s_recv, j))
                    s_out[-1].start()
            for i in range(cluster):
                for piece in range(cluster):
                    made[c, piece, i * rf : (i + 1) * rf] = reads[c * cluster + i][
                        piece * rf : (piece + 1) * rf
                    ]
            for i in reversed(range(cluster)):
                j = c * cluster + i
                if j:
                    a_out.append(to_seq(made.at[c, flip(f, i)], parts.at[j], a_send, a_recv, j))
                    a_out[-1].start()

    def arranged(tile, p):
        return jnp.concatenate(
            [tile[(t ^ p) * rf : ((t ^ p) + 1) * rf] for t in range(cluster)], axis=0
        )

    for copy in s_out:
        copy.wait_recv()
    tops, sums = [], []
    for j in range(n):
        row = jnp.broadcast_to(stats[j] if j else stat_made[0, f], (rows, size))
        tops.append(arranged(jnp.sum(jnp.where(lane == line, row, 0.0), axis=1, keepdims=True), j % cluster))
        sums.append(
            arranged(jnp.sum(jnp.where(lane == line + half, row, 0.0), axis=1, keepdims=True), j % cluster)
        )
    best = functools.reduce(jnp.maximum, tops)
    weights = [jnp.exp(top - best) for top in tops]
    total_weight = sum(w * weight_sum for w, weight_sum in zip(weights, sums))
    weights = [w / total_weight for w in weights]
    for copy in a_out:
        copy.wait_recv()
    read = weights[0] * made[0, f]
    for j in range(1, n):
        read += weights[j] * arranged(parts[j], j % cluster)
    for t in range(cluster):
        for r in range(rf):
            lhs[t : t + 1, r * size : (r + 1) * size] = read[t * rf + r : t * rf + r + 1]
    token = lhs[...].astype(jnp.bfloat16)

    for load in w_loads:
        load.wait()
    t_out = []
    for dg in reversed(range(ng)):
        out = jnp.dot(token, w_v[dg], preferred_element_type=jnp.float32)
        for t in range(cluster):
            if t == 0 and dg == 0:
                own = out[:1]
                continue
            slot = t * ng + dg
            term[slot] = out[t : t + 1]
            copy = pltpu.make_async_remote_copy(
                src_ref=term.at[slot], dst_ref=landed.at[slot],
                send_sem=t_send.at[slot], recv_sem=t_recv.at[slot],
                device_id={"seq": flip(me, t), "group": flip(mg, dg)}, device_id_type=MESH,
            )
            copy.start()
            t_out.append(copy)
    for copy in t_out:
        copy.wait_recv()
    for slot in range(1, cluster * ng):
        own += landed[slot]
    out_ref[...] = own.astype(out_ref.dtype)
    for copy in q_out + s_out + a_out + t_out:
        copy.wait_send()


def solution(mesh):
    n, ng = mesh.shape["seq"], mesh.shape["group"]

    def per_device(new_queries, stored_keys, stored_values, used_length, out_weight):
        batch, heads, stretch, size = stored_keys.shape
        group = new_queries.shape[2]
        rows = heads * group
        model = out_weight.shape[-1]
        cluster, width = CLUSTER, model // ng
        rf = rows // cluster
        dma = pltpu.SemaphoreType.DMA
        anywhere = pl.BlockSpec(memory_space=pl.ANY)
        f32, bf16 = jnp.float32, jnp.bfloat16
        return pl.pallas_call(
            functools.partial(kernel, n, ng, cluster, size ** (-0.5)),
            out_shape=pltpu.VMEM((1, width), bf16),
            in_specs=[anywhere, anywhere, anywhere, pl.BlockSpec(memory_space=pltpu.SMEM), anywhere],
            out_specs=pl.BlockSpec(memory_space=pltpu.VMEM),
            scratch_shapes=[
                pltpu.VMEM((n, rows, size), bf16),
                pltpu.VMEM(stored_keys.shape, bf16),
                pltpu.VMEM(stored_values.shape, bf16),
                pltpu.VMEM((ng, rf * size, width), bf16),
                pltpu.VMEM((n // cluster, cluster, rows, size), f32),
                pltpu.VMEM((n, rows, size), f32),
                pltpu.VMEM((n // cluster, cluster, 1, size), f32),
                pltpu.VMEM((n, 1, size), f32),
                pltpu.VMEM((8, rf * size), f32),
                pltpu.VMEM((cluster * ng, 1, width), f32),
                pltpu.VMEM((cluster * ng, 1, width), f32),
                dma, dma, dma, dma((ng,)),
                dma((n,)), dma((n,)), dma((n,)), dma((n,)), dma((n,)), dma((n,)),
                dma((cluster * ng,)), dma((cluster * ng,)),
            ],
            compiler_params=pltpu.CompilerParams(collective_id=0, has_side_effects=True),
        )(
            new_queries.reshape(rows, size),
            stored_keys,
            stored_values,
            used_length,
            out_weight.reshape(rows * size, model),
        )

    return jax.shard_map(
        per_device,
        mesh=mesh,
        in_specs=(
            P("seq", "group", None, None),
            P(None, "group", "seq", None),
            P(None, "group", "seq", None),
            P(),
            P("group", None, None, None),
        ),
        out_specs=P("seq", "group"),
        check_vma=False,
    )
```

```python
import functools

import jax
import jax.numpy as jnp
from jax import lax
from jax.experimental import pallas as pl
from jax.experimental.pallas import tpu as pltpu
from jax.sharding import PartitionSpec as P

MESH = pl.DeviceIdType.MESH
CLUSTER = 2
CHUNK = 1


def flip(index, bits):
    out, bit = index, 1
    while bit <= bits:
        if bits & bit:
            out = out + bit - 2 * bit * lax.rem(index // bit, 2)
        bit *= 2
    return out


def kernel(
    n, ng, cluster, scale,
    q_hbm, k_hbm, v_hbm, used, w_hbm, out_ref,
    q_all, k_v, v_v, w_v, made, parts, stat_made, stats, lhs, term, landed,
    q_sem, k_sem, v_sem, w_sem, q_send, q_recv, s_send, s_recv, a_send, a_recv, t_send, t_recv,
):
    me, mg = lax.axis_index("seq"), lax.axis_index("group")
    batch, heads, stretch, size = k_v.shape
    rows = q_all.shape[1]
    per_head = rows // heads
    rf = rows // cluster
    f = lax.rem(me, cluster)
    width = out_ref.shape[1]
    depth = rf * size

    q_load = pltpu.make_async_copy(q_hbm, q_all.at[0], q_sem)
    q_load.start()
    barrier = pltpu.get_barrier_semaphore()
    partners = [(j, 0) for j in range(1, n)]
    partners += [(t, dg) for t in range(cluster) for dg in range(1, ng)]
    for j, dg in reversed(partners):
        pl.semaphore_signal(
            barrier, inc=1, device_id={"seq": flip(me, j), "group": flip(mg, dg)}, device_id_type=MESH
        )

    k_load = pltpu.make_async_copy(k_hbm, k_v, k_sem)
    v_load = pltpu.make_async_copy(v_hbm, v_v, v_sem)
    w_row = pl.multiple_of(f * depth, depth)
    w_loads = [
        pltpu.make_async_copy(
            w_hbm.at[pl.ds(w_row, depth), pl.ds(pl.multiple_of(flip(mg, dg) * width, width), width)],
            w_v.at[dg],
            w_sem.at[dg],
        )
        for dg in range(ng)
    ]
    for load in [k_load, v_load] + w_loads:
        load.start()
    lhs[...] = jnp.zeros_like(lhs)
    place = me * stretch + lax.broadcasted_iota(jnp.int32, (rows, stretch), 1)
    head_of = lax.broadcasted_iota(jnp.int32, (rows, size), 0) // per_head
    lane = lax.broadcasted_iota(jnp.int32, (rows, size), 1)
    line, half = lax.broadcasted_iota(jnp.int32, (rows, size), 0), size // 2

    def to_seq(src, dst, send, recv, j):
        return pltpu.make_async_remote_copy(
            src_ref=src, dst_ref=dst, send_sem=send.at[j], recv_sem=recv.at[j],
            device_id={"seq": flip(me, j), "group": mg}, device_id_type=MESH,
        )

    q_load.wait()
    pl.semaphore_wait(barrier, len(partners))
    q_out = [to_seq(q_all.at[0], q_all.at[j], q_send, q_recv, j) for j in range(1, n)]
    for copy in q_out[::-1]:
        copy.start()
    k_load.wait()
    v_load.wait()

    a_out, s_out = [], []
    clusters = n // cluster
    for start in range(0, clusters, CHUNK):
        chunk = range(start, min(start + CHUNK, clusters))
        members = [c * cluster + i for c in chunk for i in range(cluster)]
        for j in members:
            if j:
                q_out[j - 1].wait_recv()
        logits, parts_of, tops, sums, reads = {}, {}, {}, {}, {}
        for j in members:
            b = flip(me, j)
            q = q_all[j]
            split_q = jnp.concatenate(
                [jnp.where(head_of == h, q, jnp.zeros_like(q)) for h in range(heads)], axis=1
            )
            keys = jnp.concatenate([k_v[b, h] for h in range(heads)], axis=1)
            logit = lax.dot_general(
                split_q, keys, (((1,), (1,)), ((), ())), preferred_element_type=jnp.float32
            ) * scale
            logits[j] = jnp.where(place < used[b], logit, -1e30)
        for j in members:
            tops[j] = jnp.max(logits[j], axis=1, keepdims=True)
        for j in members:
            filled = place < used[flip(me, j)]
            part = jnp.where(filled, jnp.exp(logits[j] - tops[j]), 0.0)
            high = part.astype(jnp.bfloat16)
            low = (part - high.astype(jnp.float32)).astype(jnp.bfloat16)
            parts_of[j] = jnp.concatenate([high, low], axis=0)
            sums[j] = jnp.sum(part, axis=1, keepdims=True)
        for j in members:
            b = flip(me, j)
            values = jnp.concatenate([v_v[b, h] for h in range(heads)], axis=1)
            both = jnp.dot(parts_of[j], values, preferred_element_type=jnp.float32)
            both = both[:rows] + both[rows:]
            reads[j] = jnp.concatenate(
                [
                    both[h * per_head : (h + 1) * per_head, h * size : (h + 1) * size]
                    for h in range(heads)
                ],
                axis=0,
            )
        for c in reversed(chunk):
            for piece in range(cluster):
                cut = slice(piece * rf, (piece + 1) * rf)
                pick = [c * cluster + i for i in range(cluster)]
                top = jnp.concatenate([tops[j][cut] for j in pick], axis=0)
                weight_sum = jnp.concatenate([sums[j][cut] for j in pick], axis=0)
                spread = jnp.where(lane == line, top, jnp.where(lane == line + half, weight_sum, 0.0))
                stat_made[c, piece] = jnp.sum(spread, axis=0, keepdims=True)
            for i in reversed(range(cluster)):
                j = c * cluster + i
                if j:
                    s_out.append(to_seq(stat_made.at[c, flip(f, i)], stats.at[j], s_send, s_recv, j))
                    s_out[-1].start()
            for i in range(cluster):
                for piece in range(cluster):
                    made[c, piece, i * rf : (i + 1) * rf] = reads[c * cluster + i][
                        piece * rf : (piece + 1) * rf
                    ]
            for i in reversed(range(cluster)):
                j = c * cluster + i
                if j:
                    a_out.append(to_seq(made.at[c, flip(f, i)], parts.at[j], a_send, a_recv, j))
                    a_out[-1].start()

    def arranged(tile, p):
        return jnp.concatenate(
            [tile[(t ^ p) * rf : ((t ^ p) + 1) * rf] for t in range(cluster)], axis=0
        )

    for copy in s_out:
        copy.wait_recv()
    tops, sums = [], []
    for j in range(n):
        row = jnp.broadcast_to(stats[j] if j else stat_made[0, f], (rows, size))
        tops.append(arranged(jnp.sum(jnp.where(lane == line, row, 0.0), axis=1, keepdims=True), j % cluster))
        sums.append(
            arranged(jnp.sum(jnp.where(lane == line + half, row, 0.0), axis=1, keepdims=True), j % cluster)
        )
    best = functools.reduce(jnp.maximum, tops)
    weights = [jnp.exp(top - best) for top in tops]
    total_weight = sum(w * weight_sum for w, weight_sum in zip(weights, sums))
    weights = [w / total_weight for w in weights]
    for copy in a_out:
        copy.wait_recv()
    read = weights[0] * made[0, f]
    for j in range(1, n):
        read += weights[j] * arranged(parts[j], j % cluster)
    for t in range(cluster):
        for r in range(rf):
            lhs[t : t + 1, r * size : (r + 1) * size] = read[t * rf + r : t * rf + r + 1]
    token = lhs[...].astype(jnp.bfloat16)

    for load in w_loads:
        load.wait()
    t_out = []
    for dg in [*range(ng // 2, ng), *range(ng // 2)]:
        out = jnp.dot(token, w_v[dg], preferred_element_type=jnp.float32)
        for t in range(cluster):
            if t == 0 and dg == 0:
                own = out[:1]
                continue
            slot = t * ng + dg
            term[slot] = out[t : t + 1]
            copy = pltpu.make_async_remote_copy(
                src_ref=term.at[slot], dst_ref=landed.at[slot],
                send_sem=t_send.at[slot], recv_sem=t_recv.at[slot],
                device_id={"seq": flip(me, t), "group": flip(mg, dg)}, device_id_type=MESH,
            )
            copy.start()
            t_out.append(copy)
    for copy in t_out:
        copy.wait_recv()
    for slot in range(1, cluster * ng):
        own += landed[slot]
    out_ref[...] = own.astype(out_ref.dtype)
    for copy in q_out + s_out + a_out + t_out:
        copy.wait_send()


def solution(mesh):
    n, ng = mesh.shape["seq"], mesh.shape["group"]

    def per_device(new_queries, stored_keys, stored_values, used_length, out_weight):
        batch, heads, stretch, size = stored_keys.shape
        group = new_queries.shape[2]
        rows = heads * group
        model = out_weight.shape[-1]
        cluster, width = CLUSTER, model // ng
        rf = rows // cluster
        dma = pltpu.SemaphoreType.DMA
        anywhere = pl.BlockSpec(memory_space=pl.ANY)
        f32, bf16 = jnp.float32, jnp.bfloat16
        return pl.pallas_call(
            functools.partial(kernel, n, ng, cluster, size ** (-0.5)),
            out_shape=pltpu.VMEM((1, width), bf16),
            in_specs=[anywhere, anywhere, anywhere, pl.BlockSpec(memory_space=pltpu.SMEM), anywhere],
            out_specs=pl.BlockSpec(memory_space=pltpu.VMEM),
            scratch_shapes=[
                pltpu.VMEM((n, rows, size), bf16),
                pltpu.VMEM(stored_keys.shape, bf16),
                pltpu.VMEM(stored_values.shape, bf16),
                pltpu.VMEM((ng, rf * size, width), bf16),
                pltpu.VMEM((n // cluster, cluster, rows, size), f32),
                pltpu.VMEM((n, rows, size), f32),
                pltpu.VMEM((n // cluster, cluster, 1, size), f32),
                pltpu.VMEM((n, 1, size), f32),
                pltpu.VMEM((8, rf * size), f32),
                pltpu.VMEM((cluster * ng, 1, width), f32),
                pltpu.VMEM((cluster * ng, 1, width), f32),
                dma, dma, dma, dma((ng,)),
                dma((n,)), dma((n,)), dma((n,)), dma((n,)), dma((n,)), dma((n,)),
                dma((cluster * ng,)), dma((cluster * ng,)),
            ],
            compiler_params=pltpu.CompilerParams(collective_id=0, has_side_effects=True),
        )(
            new_queries.reshape(rows, size),
            stored_keys,
            stored_values,
            used_length,
            out_weight.reshape(rows * size, model),
        )

    return jax.shard_map(
        per_device,
        mesh=mesh,
        in_specs=(
            P("seq", "group", None, None),
            P(None, "group", "seq", None),
            P(None, "group", "seq", None),
            P(),
            P("group", None, None, None),
        ),
        out_specs=P("seq", "group"),
        check_vma=False,
    )
```
